32 devices in a mesh: dp: 4 (over y, core), tp: 8 (over z, x).
Axes of the slice: x: 2, y: 2, z: 4, core: 2. Of those that a mesh axis runs over, the one named last changes fastest.
Arguments:
- inputs: bfloat16 [4, 8, 8192], P('dp', 'tp'), may hold values from -134 to 134, as said below
- norm_gain: float32 [8192], replicated, may hold values from 0.1 to 1.9
- gate_grad: bfloat16 [4, 8, 16384], P('dp', None, 'tp'), may hold values from -36 to 36
- up_grad: bfloat16 [4, 8, 16384], P('dp', None, 'tp'), may hold values from -36 to 36
- gate_weight: bfloat16 [8192, 16384], P(None, 'tp'), may hold values from -0.046875 to 0.046875
- up_weight: bfloat16 [8192, 16384], P(None, 'tp'), may hold values from -0.046875 to 0.046875
Outputs:
- input_grad: bfloat16 [4, 8, 8192], P('dp', 'tp')
- gain_grad: float32 [8192], replicated
The draws below stay inside these ranges and needn't reach their ends.
Inputs may be any that keep to these rules, and one draw needn't show every extreme that they name: `inputs`: activations with token and feature scales.
All inputs are finite; a program needn't handle non-finite values.
Results may differ from the reference program's by a relative error of at most 0.00165.
Values may be sent and summed in bfloat16 or wider, within the bound.
A program may use at most 128 MiB of HBM per device.

```python
import math
import jax
import jax.numpy as jnp
from jax import lax

D = 8192
FF = 16384
SEQ = 8
BATCH = 4


def draw_inputs(key, part):
    key_rows, key_cols, key_vals = jax.random.split(key, 3)
    row_scale = jnp.exp(jax.random.uniform(key_rows, (BATCH, SEQ, 1), jnp.float32, 0.0, math.log(10.0)))
    col_scale = jnp.exp(jax.random.uniform(key_cols, (1, 1, D), jnp.float32, 0.0, math.log(10.0)))
    sample = jnp.clip(jax.random.normal(key_vals, (BATCH, SEQ, D), jnp.float32), -4.0, 4.0)
    return (sample * row_scale * col_scale / 3.0).astype(jnp.bfloat16)


def cotangent(key, salt):
    key_cols, key_vals = jax.random.split(jax.random.fold_in(key, salt), 2)
    position = jnp.arange(SEQ, dtype=jnp.float32) / max(SEQ - 1, 1)
    col_scale = jnp.exp(jax.random.uniform(key_cols, (1, 1, FF), jnp.float32, math.log(0.3), math.log(3.0)))
    rising = 1.0 + 2.0 * position
    sample = jnp.clip(jax.random.normal(key_vals, (BATCH, SEQ, FF), jnp.float32), -4.0, 4.0)
    return (sample * rising[None, :, None] * col_scale).astype(jnp.bfloat16)


def draw_gate_grad(key, part):
    return cotangent(key, 11)


def draw_up_grad(key, part):
    return cotangent(key, 23)


def shard_levels(key, extent, cuts, smallest, top_value):
    factor_of = 1.0
    for dim, blocks in cuts:
        draws = jax.random.uniform(jax.random.fold_in(jax.random.fold_in(key, 6), dim), (blocks,), jnp.float32, smallest / len(cuts), top_value / len(cuts))
        factor_of = factor_of * jnp.repeat(jnp.exp(draws), extent[dim] // blocks).reshape((-1,) + (1,) * (len(extent) - 1 - dim))
    return factor_of


def bell_draw(key, extent, scale, most, cuts=(), held_as=jnp.bfloat16):
    values = jax.random.normal(key, extent, jnp.float32) * scale
    if len(cuts) > 0:
        values = shard_levels(key, extent, cuts, -0.22, 0.18) * values
    return jnp.clip(values, min=-most, max=most).astype(held_as)


def setup_inputs(seed: int = 0) -> dict:
    arg_keys = jax.random.split(jax.random.key(seed), 7)
    inputs = draw_inputs(jax.random.fold_in(arg_keys[6], 71), 0)
    norm_gain = jnp.clip(1.0 + 0.18 * jax.random.normal(arg_keys[1], (D,), jnp.float32), 0.1, 1.9)
    gate_grad = draw_gate_grad(jax.random.fold_in(arg_keys[6], 71), 0)
    up_grad = draw_up_grad(jax.random.fold_in(arg_keys[6], 71), 0)
    gate_weight = bell_draw(arg_keys[4], (D, FF), FF ** -0.5, 0.046875, ((1, 8),))
    up_weight = bell_draw(arg_keys[5], (D, FF), FF ** -0.5, 0.046875, ((1, 8),))
    return dict(inputs=inputs, norm_gain=norm_gain, gate_grad=gate_grad, up_grad=up_grad, gate_weight=gate_weight, up_weight=up_weight)


epsilon = 1e-05

def reference(inputs, norm_gain, gate_grad, up_grad, gate_weight, up_weight):
    values = inputs.astype(jnp.float32)
    inv_rms = lax.rsqrt(lax.optimization_barrier(jnp.mean(values * values, axis=-1, keepdims=True)) + epsilon)
    normed = values * inv_rms
    flat_gate = gate_grad.reshape(-1, gate_grad.shape[-1])
    flat_up = up_grad.reshape(-1, up_grad.shape[-1])
    dims = (((1,), (1,)), ((), ()))
    row_grad = lax.dot_general(flat_gate, gate_weight, dims, preferred_element_type=jnp.float32)
    row_grad = row_grad + lax.dot_general(flat_up, up_weight, dims, preferred_element_type=jnp.float32)
    row_grad = row_grad.reshape(inputs.shape)
    gain_grad = lax.optimization_barrier(jnp.sum(row_grad * normed, axis=(0, 1)))
    scaled = row_grad * norm_gain
    inner = lax.optimization_barrier(jnp.mean(scaled * normed, axis=-1, keepdims=True))
    input_grad = (inv_rms * (scaled - normed * inner)).astype(jnp.bfloat16)
    return (input_grad, gain_grad)
```

```python
import functools

import jax
import jax.numpy as jnp
from jax import lax
from jax.experimental import pallas as pl
from jax.experimental.pallas import tpu as pltpu
from jax.sharding import PartitionSpec as P

epsilon = 1e-05
MESH = pl.DeviceIdType.MESH
NT = (((1,), (1,)), ((), ()))


def normalize(values):
    inv_rms = lax.rsqrt(jnp.mean(values * values, axis=-1, keepdims=True) + epsilon)
    return (inv_rms, values * inv_rms)


def plain(inputs, norm_gain, gate_grad, up_grad, gate_weight, up_weight):
    seq = gate_grad.shape[1]
    width = gate_weight.shape[0]
    cot_gate = gate_grad.reshape(-1, gate_grad.shape[-1])
    cot_up = up_grad.reshape(-1, up_grad.shape[-1])
    inv_rms, normed = normalize(inputs.astype(jnp.float32))
    full_term = lax.dot_general(cot_gate, gate_weight, NT, preferred_element_type=jnp.float32)
    full_term = full_term + lax.dot_general(cot_up, up_weight, NT, preferred_element_type=jnp.float32)
    full_term = full_term.reshape(-1, seq, width)
    row_grad = lax.psum_scatter(full_term, "tp", scatter_dimension=1, tiled=True)
    gain_grad = lax.psum(jnp.sum(row_grad * normed, axis=(0, 1)), ("dp", "tp"))
    scaled = row_grad * norm_gain
    inner = jnp.mean(scaled * normed, axis=-1, keepdims=True)
    return ((inv_rms * (scaled - normed * inner)).astype(jnp.bfloat16), gain_grad)


def kernel(
    n_dp, n_tp, x_ref, gain_hbm, gg_ref, ug_ref, gw_ref, uw_ref, dx_ref, dg_ref,
    w_buf, cot, g_mat, x_row, gain_ref, x_send, x_recv, x_mat, acc, part_send, part_recv, last_send, last_recv,
    w_sem, own_sem, row_sem, known, cot_ss, cot_rs, x_ss, x_rs, part_ss, part_rs, last_ss, last_rs,
):
    n = n_dp * n_tp
    bits = n_tp.bit_length() - 1
    d, t = lax.axis_index("dp"), lax.axis_index("tp")
    me = d * n_tp + t
    seq = gg_ref.shape[1]
    width = gw_ref.shape[0]
    cut = width // n
    base = d * (n_tp * cut)

    def flip(to, k):
        for bit in range(bits):
            if k >> bit & 1:
                to = to + 2**bit - 2 ** (bit + 1) * lax.rem(lax.div(to, 2**bit), 2)
        return to

    partners = [flip(t, k) for k in range(n_tp)]
    rows_of = [lax.rem(d + step, n_dp) for step in range(n_dp)]

    own = [
        pltpu.make_async_copy(gg_ref.at[0], cot.at[d, 0], own_sem.at[0]),
        pltpu.make_async_copy(ug_ref.at[0], cot.at[d, 1], own_sem.at[1]),
        pltpu.make_async_copy(x_ref, x_row, row_sem.at[0]),
        pltpu.make_async_copy(gain_hbm, gain_ref, row_sem.at[1]),
    ]
    with jax.named_scope("own_start"):
        for copy in own:
            copy.start()

    with jax.named_scope("greet"):
        barrier = pltpu.get_barrier_semaphore()
        for bit in range(bits):
            pl.semaphore_signal(barrier, inc=1, device_id={"dp": d, "tp": partners[2**bit]}, device_id_type=MESH)
        for step in range(1, n_dp):
            pl.semaphore_signal(barrier, inc=1, device_id={"dp": rows_of[step], "tp": t}, device_id_type=MESH)


    order = sorted(range(n_tp), key=lambda k: -(k.bit_length()))
    half = n_tp // 2

    def weight_copy(i, which):
        rows = pl.ds(pl.multiple_of(base + partners[order[i]] * cut, cut), cut)
        source = (gw_ref, uw_ref)[which]
        return pltpu.make_async_copy(source.at[rows, :], w_buf.at[i, which], w_sem.at[i, which])

    stream = [(i, 0) for i in range(half)] + [(i, 1) for i in range(half)]
    stream += [(i, which) for i in range(half, n_tp) for which in range(2)]
    with jax.named_scope("w_start"):
        for i, which in stream:
            weight_copy(i, which).start()

    def cot_copy(step, which):
        to = rows_of[step]
        return pltpu.make_async_remote_copy(
            src_ref=cot.at[d, which], dst_ref=cot.at[d, which],
            send_sem=cot_ss.at[which, to], recv_sem=cot_rs.at[which, d],
            device_id={"dp": to, "tp": t}, device_id_type=MESH,
        )

    def cot_arrival(step, which):
        source = rows_of[step]
        return pltpu.make_async_remote_copy(
            src_ref=cot.at[source, which], dst_ref=cot.at[source, which],
            send_sem=cot_ss.at[which, source], recv_sem=cot_rs.at[which, source],
            device_id={"dp": source, "tp": t}, device_id_type=MESH,
        )

    with jax.named_scope("own_wait"):
        own[0].wait()
        own[1].wait()
    with jax.named_scope("bar_wait"):
        pl.semaphore_wait(barrier, bits + n_dp - 1)
    with jax.named_scope("cot_start"):
        for which in range(2):
            for step in range(1, n_dp):
                cot_copy(step, which).start()

    def tell(bit):
        pl.semaphore_signal(known.at[bit], inc=1, device_id={"dp": d, "tp": partners[2**bit]}, device_id_type=MESH)

    def part_copy(i):
        return pltpu.make_async_remote_copy(
            src_ref=part_send.at[i], dst_ref=part_recv.at[i], send_sem=part_ss.at[i], recv_sem=part_rs.at[i],
            device_id={"dp": d, "tp": partners[order[i]]}, device_id_type=MESH,
        )

    place = t * n_dp + d

    def other(k):
        flat = k + lax.div(k + n - place, n)
        to_t = lax.div(flat, n_dp)
        return flat - to_t * n_dp, to_t

    def spread(send, recv, send_sem, recv_sem, k):
        to_d, to_t = other(k)
        return pltpu.make_async_remote_copy(
            src_ref=send.at[to_d * n_tp + to_t], dst_ref=recv.at[me], send_sem=send_sem, recv_sem=recv_sem,
            device_id={"dp": to_d, "tp": to_t}, device_id_type=MESH,
        )

    def all_of(send, recv, send_sem, recv_sem):
        return pltpu.make_async_remote_copy(
            src_ref=send.at[pl.ds(0, n - 1)], dst_ref=recv.at[pl.ds(0, n - 1)], send_sem=send_sem,
            recv_sem=recv_sem, device_id={"dp": rows_of[1], "tp": t}, device_id_type=MESH,
        )

    def gather(which):
        for step in range(1, n_dp):
            cot_arrival(step, which).wait_recv()
        for row in range(n_dp):
            g_mat[which, row * seq:(row + 1) * seq, :] = cot[row, which]

    lanes = [slice(low, low + cut // 2) for low in range(0, cut, cut // 2)]

    def product(i, which, rows):
        return lax.dot_general(w_buf[i, which, rows, :], g_mat[which], NT, preferred_element_type=jnp.float32)

    tell(1)
    with jax.named_scope("x_norm"):
        own[2].wait()
        squares = jnp.zeros((1, cut), jnp.float32)
        for i in range(n):
            piece = x_row[0, :, i * cut:(i + 1) * cut].astype(jnp.float32)
            x_send[i] = piece
            squares = squares + piece * piece
        inv_rms = lax.rsqrt(jnp.sum(squares, axis=1, keepdims=True) / width + epsilon)
        for i in range(n):
            x_send[i] = x_send[i] * inv_rms
        x_recv[me] = x_send[me]
    with jax.named_scope("rounds"):
        for bit in range(1, bits):
            pl.semaphore_wait(known.at[bit], 1)
            if bit + 1 < bits:
                tell(bit + 1)
        for step in range(1, n_dp):
            pl.semaphore_signal(known.at[0], inc=1, device_id={"dp": rows_of[step], "tp": t}, device_id_type=MESH)
    with jax.named_scope("gather0"):
        gather(0)
        for i in range(half):
            weight_copy(i, 0).wait()
    with jax.named_scope("gate_far"):
        for i in range(half):
            for rows in lanes:
                acc[i, rows, :] = product(i, 0, rows)
    with jax.named_scope("known"):
        pl.semaphore_wait(known.at[0], n_dp - 1)
    with jax.named_scope("x_start"):
        for k in range(n - 1):
            spread(x_send, x_recv, x_ss, x_rs, k).start()
    with jax.named_scope("gather1"):
        gather(1)
        for i in range(half):
            weight_copy(i, 1).wait()
    with jax.named_scope("up_far"):
        for i in range(half):
            for rows in lanes:
                part_send[i, :, rows] = (acc[i, rows, :] + product(i, 1, rows)).T
            part_copy(i).start()
    with jax.named_scope("w_wait"):
        for i in range(half, n_tp):
            for which in range(2):
                weight_copy(i, which).wait()
    with jax.named_scope("near"):
        for i in range(half, n_tp):
            for rows in lanes:
                part_send[i, :, rows] = (product(i, 0, rows) + product(i, 1, rows)).T
            if i < n_tp - 1:
                part_copy(i).start()
    total = part_send[n_tp - 1]

    with jax.named_scope("x_wait"):
        all_of(x_send, x_recv, x_ss, x_rs).wait_recv()
    with jax.named_scope("x_mat"):
        for i in range(n):
            x_mat[i:i + 1, :] = x_recv[i]

    for i in reversed(range(n_tp - 1)):
        with jax.named_scope(f"part{i}"):
            part_copy(i).wait_recv()
            total = total + part_recv[i]

    with jax.named_scope("gain_part"):
        gain_part = jnp.sum(total * x_mat[...], axis=0, keepdims=True)
        for i in range(n):
            last_send[i, 0] = total[i:i + 1, :]
            last_send[i, 1] = gain_part
    with jax.named_scope("last_start"):
        for k in range(n - 1):
            spread(last_send, last_recv, last_ss, last_rs, k).start()

        last_recv[me] = last_send[me]

    with jax.named_scope("send_waits"):
        own[3].wait()
        for which in range(2):
            for step in range(1, n_dp):
                cot_copy(step, which).wait_send()
        for i in range(n_tp - 1):
            part_copy(i).wait_send()
        all_of(x_send, x_recv, x_ss, x_rs).wait_send()
        all_of(last_send, last_recv, last_ss, last_rs).wait_send()

    with jax.named_scope("last_wait"):
        all_of(last_send, last_recv, last_ss, last_rs).wait_recv()

    with jax.named_scope("finish"):
        dots = jnp.zeros((1, cut), jnp.float32)
        for i in range(n):
            dots = dots + last_recv[i, 0] * gain_ref[i] * x_send[i]
            dg_ref[i] = last_recv[i, 1]
        inner = jnp.sum(dots, axis=1, keepdims=True) / width
        for i in range(n):
            scaled = last_recv[i, 0] * gain_ref[i]
            dx_ref[0, :, i * cut:(i + 1) * cut] = (inv_rms * (scaled - x_send[i] * inner)).astype(jnp.bfloat16)


def write_out(dx_ref, dg_ref, dx_out, dg_out):
    dx_out[...] = dx_ref[...]
    dg_out[...] = dg_ref[...]


def fused(n_dp, n_tp, inputs, norm_gain, gate_grad, up_grad, gate_weight, up_weight):
    n = n_dp * n_tp
    seq, depth = gate_grad.shape[1:]
    width = gate_weight.shape[0]
    cut = width // n
    rows = n_dp * seq
    dma, vmem = pltpu.SemaphoreType.DMA, pltpu.VMEM
    input_grad, gain_grad = pl.pallas_call(
        functools.partial(kernel, n_dp, n_tp),
        out_shape=(vmem(inputs.shape, jnp.bfloat16), vmem((n, 1, cut), jnp.float32)),
        in_specs=[pl.BlockSpec(memory_space=pl.ANY)] * 6,
        out_specs=(pl.BlockSpec(memory_space=vmem),) * 2,
        scratch_shapes=[
            vmem((n_tp, 2, cut, depth), jnp.bfloat16),
            vmem((n_dp, 2, seq, depth), jnp.bfloat16),
            vmem((2, rows, depth), jnp.bfloat16),
            vmem(inputs.shape, jnp.bfloat16),
            vmem((n, 1, cut), jnp.float32),
            vmem((n, 1, cut), jnp.float32),
            vmem((n, 1, cut), jnp.float32),
            vmem((n, cut), jnp.float32),
            vmem((n_tp // 2, cut, rows), jnp.float32),
            vmem((n_tp, rows, cut), jnp.float32),
            vmem((n_tp, rows, cut), jnp.float32),
            vmem((n, 2, 1, cut), jnp.float32),
            vmem((n, 2, 1, cut), jnp.float32),
            dma((n_tp, 2)), dma((2,)), dma((2,)),
            pltpu.SemaphoreType.REGULAR((n_tp.bit_length(),)),
            dma((2, n_dp)), dma((2, n_dp)),
            dma, dma,
            dma((n_tp,)), dma((n_tp,)),
            dma, dma,
        ],
        compiler_params=pltpu.CompilerParams(collective_id=0, has_side_effects=True),
    )(inputs, norm_gain.reshape(n, 1, cut), gate_grad, up_grad, gate_weight, up_weight)
    input_grad, gain_grad = pl.pallas_call(
        write_out,
        out_shape=(
            jax.ShapeDtypeStruct(inputs.shape, jnp.bfloat16),
            jax.ShapeDtypeStruct((n, 1, cut), jnp.float32),
        ),
        in_specs=[pl.BlockSpec(memory_space=vmem)] * 2,
        out_specs=(pl.BlockSpec(memory_space=vmem),) * 2,
        compiler_params=pltpu.CompilerParams(vmem_limit_bytes=2**20),
    )(input_grad, gain_grad)
    return (input_grad, gain_grad.reshape(width))


def per_device(n_dp, n_tp, *args):
    inputs, gate_grad, gate_weight = args[0], args[2], args[4]
    n = n_dp * n_tp
    width, depth = gate_weight.shape
    fits = (
        inputs.shape[:2] == (1, 1)
        and gate_grad.shape[0] == 1
        and gate_grad.shape[1] == n_tp
        and n_tp % 8 == 0
        and n_tp & (n_tp - 1) == 0
        and width % (n * 128) == 0
        and depth % 256 == 0
        and width // n_dp * depth * 4 <= 40 * 2**20
    )
    return fused(n_dp, n_tp, *args) if fits else plain(*args)


def solution(mesh):
    return jax.shard_map(
        functools.partial(per_device, mesh.shape["dp"], mesh.shape["tp"]),
        mesh=mesh,
        in_specs=(
            P("dp", "tp", None),
            P(),
            P("dp", None, "tp"),
            P("dp", None, "tp"),
            P(None, "tp"),
            P(None, "tp"),
        ),
        out_specs=(P("dp", "tp", None), P()),
        check_vma=False,
    )
```

```python
import functools

import jax
import jax.numpy as jnp
from jax import lax
from jax.experimental import pallas as pl
from jax.experimental.pallas import tpu as pltpu
from jax.sharding import PartitionSpec as P

epsilon = 1e-05
MESH = pl.DeviceIdType.MESH
NT = (((1,), (1,)), ((), ()))


def normalize(values):
    inv_rms = lax.rsqrt(jnp.mean(values * values, axis=-1, keepdims=True) + epsilon)
    return (inv_rms, values * inv_rms)


def plain(inputs, norm_gain, gate_grad, up_grad, gate_weight, up_weight):
    seq = gate_grad.shape[1]
    width = gate_weight.shape[0]
    cot_gate = gate_grad.reshape(-1, gate_grad.shape[-1])
    cot_up = up_grad.reshape(-1, up_grad.shape[-1])
    inv_rms, normed = normalize(inputs.astype(jnp.float32))
    full_term = lax.dot_general(cot_gate, gate_weight, NT, preferred_element_type=jnp.float32)
    full_term = full_term + lax.dot_general(cot_up, up_weight, NT, preferred_element_type=jnp.float32)
    full_term = full_term.reshape(-1, seq, width)
    row_grad = lax.psum_scatter(full_term, "tp", scatter_dimension=1, tiled=True)
    gain_grad = lax.psum(jnp.sum(row_grad * normed, axis=(0, 1)), ("dp", "tp"))
    scaled = row_grad * norm_gain
    inner = jnp.mean(scaled * normed, axis=-1, keepdims=True)
    return ((inv_rms * (scaled - normed * inner)).astype(jnp.bfloat16), gain_grad)


def kernel(
    n_dp, n_tp, x_ref, gain_hbm, gg_ref, ug_ref, gw_ref, uw_ref, dx_ref, dg_ref,
    w_buf, cot, g_mat, x_row, gain_ref, x_send, x_recv, x_mat, acc, mine, scale_send, scale_recv, part_send, part_recv, last_send, last_recv,
    w_sem, own_sem, known, cot_ss, cot_rs, x_ss, x_rs, part_ss, part_rs, last_ss, last_rs,
):
    n = n_dp * n_tp
    bits = n_tp.bit_length() - 1
    d, t = lax.axis_index("dp"), lax.axis_index("tp")
    me = d * n_tp + t
    seq = gg_ref.shape[1]
    width = gw_ref.shape[0]
    cut = width // n
    base = d * (n_tp * cut)

    def flip(to, k):
        for bit in range(bits):
            if k >> bit & 1:
                to = to + 2**bit - 2 ** (bit + 1) * lax.rem(lax.div(to, 2**bit), 2)
        return to

    partners = [flip(t, k) for k in range(n_tp)]
    rows_of = [lax.rem(d + step, n_dp) for step in range(n_dp)]

    own = [
        pltpu.make_async_copy(gg_ref.at[0], cot.at[0, d], own_sem.at[0]),
        pltpu.make_async_copy(ug_ref.at[0], cot.at[1, d], own_sem.at[1]),
        pltpu.make_async_copy(x_ref, x_row, own_sem.at[2]),
        pltpu.make_async_copy(gain_hbm, gain_ref, own_sem.at[3]),
    ]
    with jax.named_scope("own_start"):
        for copy in own:
            copy.start(priority=1)

    with jax.named_scope("greet"):
        barrier = pltpu.get_barrier_semaphore()
        for bit in range(bits):
            pl.semaphore_signal(barrier, inc=1, device_id={"dp": d, "tp": partners[2**bit]}, device_id_type=MESH)
        for step in range(1, n_dp):
            pl.semaphore_signal(barrier, inc=1, device_id={"dp": rows_of[step], "tp": t}, device_id_type=MESH)


    order = sorted(range(n_tp), key=lambda k: -(k.bit_length()))
    half = n_tp // 2

    def first_far(i, which):
        return i < half and which == 0

    def weight_copy(i, which):
        rows = pl.ds(pl.multiple_of(base + partners[order[i]] * cut, cut), cut)
        source = (gw_ref, uw_ref)[which]
        slot = pl.ds((which * n_tp + i) * cut, cut)
        return pltpu.make_async_copy(source.at[rows, :], w_buf.at[slot, :], w_sem.at[0 if first_far(i, which) else 1])

    def weights_here(which):
        low, count = ((0, half), (half, 2 * n_tp - half))[which]
        return pltpu.make_async_copy(
            gw_ref.at[pl.ds(0, count * cut), :], w_buf.at[pl.ds(low * cut, count * cut), :], w_sem.at[which]
        )

    stream = [(i, 0) for i in range(half)] + [(i, 1) for i in range(half)]
    stream += [(i, which) for i in range(half, n_tp) for which in range(2)]
    with jax.named_scope("w_start"):
        for i, which in stream:
            weight_copy(i, which).start()

    def cot_copy(step, which):
        to = rows_of[step]
        return pltpu.make_async_remote_copy(
            src_ref=cot.at[which, d], dst_ref=cot.at[which, d], send_sem=cot_ss, recv_sem=cot_rs.at[which],
            device_id={"dp": to, "tp": t}, device_id_type=MESH,
        )

    def cots(which):
        return pltpu.make_async_remote_copy(
            src_ref=cot.at[which, pl.ds(0, n_dp - 1)], dst_ref=cot.at[which, pl.ds(0, n_dp - 1)], send_sem=cot_ss,
            recv_sem=cot_rs.at[which], device_id={"dp": rows_of[1], "tp": t}, device_id_type=MESH,
        )

    with jax.named_scope("own_wait"):
        own[0].wait()
        own[1].wait()
    with jax.named_scope("bar_wait"):
        pl.semaphore_wait(barrier, bits + n_dp - 1)
    with jax.named_scope("cot_start"):
        for which in range(2):
            for step in range(1, n_dp):
                cot_copy(step, which).start()

    def tell(bit):
        pl.semaphore_signal(known.at[bit], inc=1, device_id={"dp": d, "tp": partners[2**bit]}, device_id_type=MESH)

    groups = [(0, half), (half, n_tp - 2), (n_tp - 2, n_tp - 1)]

    def part_copies(i):
        group = [low <= i < high for low, high in groups].index(True)
        return [
            pltpu.make_async_remote_copy(
                src_ref=send.at[i], dst_ref=recv.at[i], send_sem=part_ss.at[which], recv_sem=part_rs.at[which, group],
                device_id={"dp": d, "tp": partners[order[i]]}, device_id_type=MESH,
            )
            for which, (send, recv) in enumerate(((scale_send, scale_recv), (part_send, part_recv)))
        ]

    def parts(low, high, group):
        return [
            pltpu.make_async_remote_copy(
                src_ref=send.at[pl.ds(low, high - low)], dst_ref=recv.at[pl.ds(low, high - low)],
                send_sem=part_ss.at[which], recv_sem=part_rs.at[which, group],
                device_id={"dp": d, "tp": partners[1]}, device_id_type=MESH,
            )
            for which, (send, recv) in enumerate(((scale_send, scale_recv), (part_send, part_recv)))
        ]

    place = t * n_dp + d

    def other(k):
        flat = k + lax.div(k + n - place, n)
        to_t = lax.div(flat, n_dp)
        return flat - to_t * n_dp, to_t

    def spread(send, recv, send_sem, recv_sem, k):
        to_d, to_t = other(k)
        return pltpu.make_async_remote_copy(
            src_ref=send.at[to_d * n_tp + to_t], dst_ref=recv.at[me], send_sem=send_sem, recv_sem=recv_sem,
            device_id={"dp": to_d, "tp": to_t}, device_id_type=MESH,
        )

    def all_of(send, recv, send_sem, recv_sem):
        return pltpu.make_async_remote_copy(
            src_ref=send.at[pl.ds(0, n - 1)], dst_ref=recv.at[pl.ds(0, n - 1)], send_sem=send_sem,
            recv_sem=recv_sem, device_id={"dp": rows_of[1], "tp": t}, device_id_type=MESH,
        )

    def gather(which):
        cots(which).wait_recv()
        for row in range(n_dp):
            g_mat[which, row * seq:(row + 1) * seq, :] = cot[which, row]

    def encode(i, cols, part):
        most = jnp.maximum(jnp.max(jnp.abs(part), axis=0, keepdims=True), 1e-30)
        scale_send[i, :, cols] = most * 2.0**-15
        root = part * (2.0**15 / most)
        square = root * root
        fourth = square * square
        part_send[i, :, cols] = (fourth * square * root * jnp.abs(root)).astype(jnp.bfloat16)

    def decode(i):
        power = part_recv[i].astype(jnp.float32)
        back = lax.rsqrt(lax.rsqrt(lax.rsqrt(jnp.maximum(jnp.abs(power), 2.0**-126))))
        square = back * back
        return power * (square * square * square * back) * scale_recv[i]

    lanes = [slice(low, low + cut // 2) for low in range(0, cut, cut // 2)]

    def product(i, which, rows):
        low = (which * n_tp + i) * cut + rows.start
        return lax.dot_general(w_buf[low:low + cut // 2, :], g_mat[which], NT, preferred_element_type=jnp.float32)

    tell(1)
    with jax.named_scope("x_norm"):
        own[2].wait()
        squares = jnp.zeros((1, cut), jnp.float32)
        for i in range(n):
            piece = x_row[0, :, i * cut:(i + 1) * cut].astype(jnp.float32)
            x_send[i] = piece
            squares = squares + piece * piece
        inv_rms = lax.rsqrt(jnp.sum(squares, axis=1, keepdims=True) / width + epsilon)
        for i in range(n):
            x_send[i] = x_send[i] * inv_rms
        x_recv[me] = x_send[me]
    with jax.named_scope("rounds"):
        for bit in range(1, bits):
            pl.semaphore_wait(known.at[bit], 1)
            if bit + 1 < bits:
                tell(bit + 1)
        for step in range(1, n_dp):
            pl.semaphore_signal(known.at[0], inc=1, device_id={"dp": rows_of[step], "tp": t}, device_id_type=MESH)
    with jax.named_scope("gather0"):
        gather(0)
        weights_here(0).wait()
    with jax.named_scope("gate_far"):
        for i in range(half):
            for rows in lanes:
                acc[i, rows, :] = product(i, 0, rows)
    with jax.named_scope("x_start"):
        pl.semaphore_wait(known.at[0], n_dp - 1)
        for k in range(n - 1):
            spread(x_send, x_recv, x_ss, x_rs, k).start()
    with jax.named_scope("gather1"):
        gather(1)
        weights_here(1).wait()
    with jax.named_scope("products"):
        for i in range(half):
            for rows in lanes:
                encode(i, rows, (acc[i, rows, :] + product(i, 1, rows)).T)
            for copy in part_copies(i):
                copy.start()
        for i in range(half, n_tp):
            for rows in lanes:
                part = (product(i, 0, rows) + product(i, 1, rows)).T
                if i < n_tp - 1:
                    encode(i, rows, part)
                else:
                    mine[:, rows] = part
            if i < n_tp - 1:
                for copy in part_copies(i):
                    copy.start()
    total = mine[...]

    with jax.named_scope("x_wait"):
        all_of(x_send, x_recv, x_ss, x_rs).wait_recv()
    with jax.named_scope("x_mat"):
        for i in range(n):
            x_mat[i:i + 1, :] = x_recv[i]

    for group, (low, high) in enumerate(groups):
        with jax.named_scope(f"part{group}"):
            for copy in parts(low, high, group):
                copy.wait_recv()
            for i in range(low, high):
                total = total + decode(i)

    with jax.named_scope("gain_part"):
        gain_part = jnp.sum(total * x_mat[...], axis=0, keepdims=True)
        for i in range(n):
            last_send[i, 0] = total[i:i + 1, :]
            last_send[i, 1] = gain_part
    with jax.named_scope("last_start"):
        for k in range(n - 1):
            spread(last_send, last_recv, last_ss, last_rs, k).start()

        last_recv[me] = last_send[me]

    with jax.named_scope("send_waits"):
        own[3].wait()
        for which in range(2):
            cots(which).wait_send()
        for copy in parts(0, n_tp - 1, 0):
            copy.wait_send()
        all_of(x_send, x_recv, x_ss, x_rs).wait_send()
        all_of(last_send, last_recv, last_ss, last_rs).wait_send()

    with jax.named_scope("last_wait"):
        all_of(last_send, last_recv, last_ss, last_rs).wait_recv()

    with jax.named_scope("finish"):
        dots = jnp.zeros((1, cut), jnp.float32)
        for i in range(n):
            dots = dots + last_recv[i, 0] * gain_ref[i] * x_send[i]
            dg_ref[i] = last_recv[i, 1]
        inner = jnp.sum(dots, axis=1, keepdims=True) / width
        for i in range(n):
            scaled = last_recv[i, 0] * gain_ref[i]
            dx_ref[0, :, i * cut:(i + 1) * cut] = (inv_rms * (scaled - x_send[i] * inner)).astype(jnp.bfloat16)


def write_out(dx_ref, dg_ref, dx_out, dg_out):
    dx_out[...] = dx_ref[...]
    dg_out[...] = dg_ref[...]


def fused(n_dp, n_tp, inputs, norm_gain, gate_grad, up_grad, gate_weight, up_weight):
    n = n_dp * n_tp
    seq, depth = gate_grad.shape[1:]
    width = gate_weight.shape[0]
    cut = width // n
    rows = n_dp * seq
    dma, vmem = pltpu.SemaphoreType.DMA, pltpu.VMEM
    input_grad, gain_grad = pl.pallas_call(
        functools.partial(kernel, n_dp, n_tp),
        out_shape=(vmem(inputs.shape, jnp.bfloat16), vmem((n, 1, cut), jnp.float32)),
        in_specs=[pl.BlockSpec(memory_space=pl.ANY)] * 6,
        out_specs=(pl.BlockSpec(memory_space=vmem),) * 2,
        scratch_shapes=[
            vmem((2 * n_tp * cut, depth), jnp.bfloat16),
            vmem((2, n_dp, seq, depth), jnp.bfloat16),
            vmem((2, rows, depth), jnp.bfloat16),
            vmem(inputs.shape, jnp.bfloat16),
            vmem((n, 1, cut), jnp.float32),
            vmem((n, 1, cut), jnp.float32),
            vmem((n, 1, cut), jnp.float32),
            vmem((n, cut), jnp.float32),
            vmem((n_tp // 2, cut, rows), jnp.float32),
            vmem((rows, cut), jnp.float32),
            vmem((n_tp, 1, cut), jnp.float32),
            vmem((n_tp, 1, cut), jnp.float32),
            vmem((n_tp, rows, cut), jnp.bfloat16),
            vmem((n_tp, rows, cut), jnp.bfloat16),
            vmem((n, 2, 1, cut), jnp.float32),
            vmem((n, 2, 1, cut), jnp.float32),
            dma((2,)), dma((4,)),
            pltpu.SemaphoreType.REGULAR((n_tp.bit_length() - 1,)),
            dma, dma((2,)),
            dma, dma,
            dma((2,)), dma((2, 3)),
            dma, dma,
        ],
        compiler_params=pltpu.CompilerParams(collective_id=0, has_side_effects=True),
    )(inputs, norm_gain.reshape(n, 1, cut), gate_grad, up_grad, gate_weight, up_weight)
    input_grad, gain_grad = pl.pallas_call(
        write_out,
        out_shape=(
            jax.ShapeDtypeStruct(inputs.shape, jnp.bfloat16),
            jax.ShapeDtypeStruct((n, 1, cut), jnp.float32),
        ),
        in_specs=[pl.BlockSpec(memory_space=vmem)] * 2,
        out_specs=(pl.BlockSpec(memory_space=vmem),) * 2,
        compiler_params=pltpu.CompilerParams(vmem_limit_bytes=2**20),
    )(input_grad, gain_grad)
    return (input_grad, gain_grad.reshape(width))


def per_device(n_dp, n_tp, *args):
    inputs, gate_grad, gate_weight = args[0], args[2], args[4]
    n = n_dp * n_tp
    width, depth = gate_weight.shape
    fits = (
        inputs.shape[:2] == (1, 1)
        and gate_grad.shape[0] == 1
        and gate_grad.shape[1] == n_tp
        and n_tp % 8 == 0
        and n_tp & (n_tp - 1) == 0
        and width % (n * 128) == 0
        and depth % 256 == 0
        and width // n_dp * depth * 4 <= 40 * 2**20
    )
    return fused(n_dp, n_tp, *args) if fits else plain(*args)


def solution(mesh):
    return jax.shard_map(
        functools.partial(per_device, mesh.shape["dp"], mesh.shape["tp"]),
        mesh=mesh,
        in_specs=(
            P("dp", "tp", None),
            P(),
            P("dp", None, "tp"),
            P("dp", None, "tp"),
            P(None, "tp"),
            P(None, "tp"),
        ),
        out_specs=(P("dp", "tp", None), P()),
        check_vma=False,
    )
```

```python
import functools

import jax
import jax.numpy as jnp
from jax import lax
from jax.experimental import pallas as pl
from jax.experimental.pallas import tpu as pltpu
from jax.sharding import PartitionSpec as P

epsilon = 1e-05
MESH = pl.DeviceIdType.MESH
NT = (((1,), (1,)), ((), ()))


def normalize(values):
    inv_rms = lax.rsqrt(jnp.mean(values * values, axis=-1, keepdims=True) + epsilon)
    return (inv_rms, values * inv_rms)


def plain(inputs, norm_gain, gate_grad, up_grad, gate_weight, up_weight):
    seq = gate_grad.shape[1]
    width = gate_weight.shape[0]
    cot_gate = gate_grad.reshape(-1, gate_grad.shape[-1])
    cot_up = up_grad.reshape(-1, up_grad.shape[-1])
    inv_rms, normed = normalize(inputs.astype(jnp.float32))
    full_term = lax.dot_general(cot_gate, gate_weight, NT, preferred_element_type=jnp.float32)
    full_term = full_term + lax.dot_general(cot_up, up_weight, NT, preferred_element_type=jnp.float32)
    full_term = full_term.reshape(-1, seq, width)
    row_grad = lax.psum_scatter(full_term, "tp", scatter_dimension=1, tiled=True)
    gain_grad = lax.psum(jnp.sum(row_grad * normed, axis=(0, 1)), ("dp", "tp"))
    scaled = row_grad * norm_gain
    inner = jnp.mean(scaled * normed, axis=-1, keepdims=True)
    return ((inv_rms * (scaled - normed * inner)).astype(jnp.bfloat16), gain_grad)


def kernel(
    n_dp, n_tp, x_ref, gain_hbm, gg_ref, ug_ref, gw_ref, uw_ref, dx_ref, dg_ref,
    w_buf, cot, g_mat, x_row, gain_ref, x_send, x_recv, x_mat, acc, mine, scale_send, scale_recv, part_send, part_recv, last_send, last_recv,
    w_sem, own_sem, known, cot_ss, cot_rs, x_ss, x_rs, part_ss, part_rs, last_ss, last_rs,
):
    n = n_dp * n_tp
    bits = n_tp.bit_length() - 1
    d, t = lax.axis_index("dp"), lax.axis_index("tp")
    me = d * n_tp + t
    seq = gg_ref.shape[1]
    width = gw_ref.shape[0]
    cut = width // n
    base = d * (n_tp * cut)

    def flip(to, k):
        for bit in range(bits):
            if k >> bit & 1:
                to = to + 2**bit - 2 ** (bit + 1) * lax.rem(lax.div(to, 2**bit), 2)
        return to

    partners = [flip(t, k) for k in range(n_tp)]
    rows_of = [lax.rem(d + step, n_dp) for step in range(n_dp)]

    own = [
        pltpu.make_async_copy(gg_ref.at[0], cot.at[0, d], own_sem.at[0]),
        pltpu.make_async_copy(ug_ref.at[0], cot.at[1, d], own_sem.at[1]),
        pltpu.make_async_copy(x_ref, x_row, own_sem.at[2]),
        pltpu.make_async_copy(gain_hbm, gain_ref, own_sem.at[3]),
    ]
    with jax.named_scope("own_start"):
        for copy in own:
            copy.start(priority=1)

    spot, line = lax.div(t, 2), n_tp // 2
    beside = lax.min(spot, 1) + lax.min(line - 1 - spot, 1)

    def signal(sem, to_d, to_t):
        pl.semaphore_signal(sem, inc=1, device_id={"dp": to_d, "tp": to_t}, device_id_type=MESH)

    def signal_line(sem):
        @pl.when(spot > 0)
        def _():
            signal(sem, d, t - 2)

        @pl.when(spot < line - 1)
        def _():
            signal(sem, d, t + 2)

    with jax.named_scope("greet"):
        barrier = pltpu.get_barrier_semaphore()
        for step in range(1, n_dp):
            signal(barrier, rows_of[step], t)
        signal(barrier, d, partners[1])
        signal_line(barrier)

    order = sorted(range(n_tp), key=lambda k: -(k.bit_length()))
    half = n_tp // 2

    def first_far(i, which):
        return i < half and which == 0

    def weight_copy(i, which):
        rows = pl.ds(pl.multiple_of(base + partners[order[i]] * cut, cut), cut)
        source = (gw_ref, uw_ref)[which]
        slot = pl.ds((which * n_tp + i) * cut, cut)
        return pltpu.make_async_copy(source.at[rows, :], w_buf.at[slot, :], w_sem.at[0 if first_far(i, which) else 1])

    def weights_here(which):
        low, count = ((0, half), (half, 2 * n_tp - half))[which]
        return pltpu.make_async_copy(
            gw_ref.at[pl.ds(0, count * cut), :], w_buf.at[pl.ds(low * cut, count * cut), :], w_sem.at[which]
        )

    stream = [(i, 0) for i in range(half)] + [(i, 1) for i in range(half)]
    stream += [(i, which) for i in range(half, n_tp) for which in range(2)]
    with jax.named_scope("w_start"):
        for i, which in stream:
            weight_copy(i, which).start()

    def cot_copy(step, which):
        to = rows_of[step]
        return pltpu.make_async_remote_copy(
            src_ref=cot.at[which, d], dst_ref=cot.at[which, d], send_sem=cot_ss, recv_sem=cot_rs.at[which],
            device_id={"dp": to, "tp": t}, device_id_type=MESH,
        )

    def cots(which):
        return pltpu.make_async_remote_copy(
            src_ref=cot.at[which, pl.ds(0, n_dp - 1)], dst_ref=cot.at[which, pl.ds(0, n_dp - 1)], send_sem=cot_ss,
            recv_sem=cot_rs.at[which], device_id={"dp": rows_of[1], "tp": t}, device_id_type=MESH,
        )

    with jax.named_scope("own_wait"):
        own[0].wait()
        own[1].wait()
    with jax.named_scope("bar_wait"):
        pl.semaphore_wait(barrier, n_dp + beside)
    with jax.named_scope("cot_start"):
        for which in range(2):
            for step in range(1, n_dp):
                cot_copy(step, which).start()

    groups = [(0, half), (half, n_tp - 2), (n_tp - 2, n_tp - 1)]

    def part_copies(i):
        group = [low <= i < high for low, high in groups].index(True)
        return [
            pltpu.make_async_remote_copy(
                src_ref=send.at[i], dst_ref=recv.at[i], send_sem=part_ss.at[which], recv_sem=part_rs.at[which, group],
                device_id={"dp": d, "tp": partners[order[i]]}, device_id_type=MESH,
            )
            for which, (send, recv) in enumerate(((scale_send, scale_recv), (part_send, part_recv)))
        ]

    def parts(low, high, group):
        return [
            pltpu.make_async_remote_copy(
                src_ref=send.at[pl.ds(low, high - low)], dst_ref=recv.at[pl.ds(low, high - low)],
                send_sem=part_ss.at[which], recv_sem=part_rs.at[which, group],
                device_id={"dp": d, "tp": partners[1]}, device_id_type=MESH,
            )
            for which, (send, recv) in enumerate(((scale_send, scale_recv), (part_send, part_recv)))
        ]

    place = t * n_dp + d

    def other(k):
        flat = k + lax.div(k + n - place, n)
        to_t = lax.div(flat, n_dp)
        return flat - to_t * n_dp, to_t

    def spread(send, recv, send_sem, recv_sem, k):
        to_d, to_t = other(k)
        return pltpu.make_async_remote_copy(
            src_ref=send.at[to_d * n_tp + to_t], dst_ref=recv.at[me], send_sem=send_sem, recv_sem=recv_sem,
            device_id={"dp": to_d, "tp": to_t}, device_id_type=MESH,
        )

    def all_of(send, recv, send_sem, recv_sem):
        return pltpu.make_async_remote_copy(
            src_ref=send.at[pl.ds(0, n - 1)], dst_ref=recv.at[pl.ds(0, n - 1)], send_sem=send_sem,
            recv_sem=recv_sem, device_id={"dp": rows_of[1], "tp": t}, device_id_type=MESH,
        )

    def gather(which):
        cots(which).wait_recv()
        for row in range(n_dp):
            g_mat[which, row * seq:(row + 1) * seq, :] = cot[which, row]

    def encode(i, cols, part):
        most = jnp.maximum(jnp.max(jnp.abs(part), axis=0, keepdims=True), 1e-30)
        scale_send[i, :, cols] = most * 2.0**-15
        root = part * (2.0**15 / most)
        square = root * root
        fourth = square * square
        part_send[i, :, cols] = (fourth * square * root * jnp.abs(root)).astype(jnp.bfloat16)

    def decode(i):
        power = part_recv[i].astype(jnp.float32)
        back = lax.rsqrt(lax.rsqrt(lax.rsqrt(jnp.maximum(jnp.abs(power), 2.0**-126))))
        square = back * back
        return power * (square * square * square * back) * scale_recv[i]

    lanes = [slice(low, low + cut // 2) for low in range(0, cut, cut // 2)]

    def product(i, which, rows):
        low = (which * n_tp + i) * cut + rows.start
        return lax.dot_general(w_buf[low:low + cut // 2, :], g_mat[which], NT, preferred_element_type=jnp.float32)

    signal_line(known.at[1])
    signal(known.at[1], d, partners[1])
    with jax.named_scope("x_norm"):
        own[2].wait()
        squares = jnp.zeros((1, cut), jnp.float32)
        for i in range(n):
            piece = x_row[0, :, i * cut:(i + 1) * cut].astype(jnp.float32)
            x_send[i] = piece
            squares = squares + piece * piece
        inv_rms = lax.rsqrt(jnp.sum(squares, axis=1, keepdims=True) / width + epsilon)
        for i in range(n):
            x_send[i] = x_send[i] * inv_rms
        x_recv[me] = x_send[me]
    with jax.named_scope("rounds"):
        for step in range(1, line - 1):
            pl.semaphore_wait(known.at[step], beside + (1 if step == 1 else 0))
            if step + 1 < line - 1:
                signal_line(known.at[step + 1])
        for step in range(n_dp):
            for side in range(2):
                if step or side:
                    signal(known.at[0], rows_of[step], partners[side])
    with jax.named_scope("gather0"):
        gather(0)
        weights_here(0).wait()
    with jax.named_scope("gate_far"):
        for i in range(half):
            for rows in lanes:
                acc[i, rows, :] = product(i, 0, rows)
    with jax.named_scope("x_start"):
        pl.semaphore_wait(known.at[0], 2 * n_dp - 1)
        for k in range(n - 1):
            spread(x_send, x_recv, x_ss, x_rs, k).start()
    with jax.named_scope("gather1"):
        gather(1)
        weights_here(1).wait()
    with jax.named_scope("products"):
        for low, high in ((0, half), (half, n_tp - 1), (n_tp - 1, n_tp)):
            for i in range(low, high):
                for rows in lanes:
                    if i < half:
                        part = (acc[i, rows, :] + product(i, 1, rows)).T
                    else:
                        part = (product(i, 0, rows) + product(i, 1, rows)).T
                    if i < n_tp - 1:
                        encode(i, rows, part)
                    else:
                        mine[:, rows] = part
            for i in range(low, min(high, n_tp - 1)):
                for copy in part_copies(i):
                    copy.start()
    total = mine[...]

    with jax.named_scope("x_wait"):
        all_of(x_send, x_recv, x_ss, x_rs).wait_recv()
    with jax.named_scope("x_mat"):
        for i in range(n):
            x_mat[i:i + 1, :] = x_recv[i]

    for group, (low, high) in enumerate(groups):
        with jax.named_scope(f"part{group}"):
            for copy in parts(low, high, group):
                copy.wait_recv()
            for i in range(low, high):
                total = total + decode(i)

    with jax.named_scope("gain_part"):
        gain_part = jnp.sum(total * x_mat[...], axis=0, keepdims=True)
        for i in range(n):
            last_send[i, 0] = total[i:i + 1, :]
            last_send[i, 1] = gain_part
    with jax.named_scope("last_start"):
        for k in range(n - 1):
            spread(last_send, last_recv, last_ss, last_rs, k).start()

        last_recv[me] = last_send[me]

    with jax.named_scope("send_waits"):
        own[3].wait()
        for which in range(2):
            cots(which).wait_send()
        for copy in parts(0, n_tp - 1, 0):
            copy.wait_send()
        all_of(x_send, x_recv, x_ss, x_rs).wait_send()
        all_of(last_send, last_recv, last_ss, last_rs).wait_send()

    with jax.named_scope("last_wait"):
        all_of(last_send, last_recv, last_ss, last_rs).wait_recv()

    with jax.named_scope("finish"):
        dots = jnp.zeros((1, cut), jnp.float32)
        for i in range(n):
            dots = dots + last_recv[i, 0] * gain_ref[i] * x_send[i]
            dg_ref[i] = last_recv[i, 1]
        inner = jnp.sum(dots, axis=1, keepdims=True) / width
        for i in range(n):
            scaled = last_recv[i, 0] * gain_ref[i]
            dx_ref[0, :, i * cut:(i + 1) * cut] = (inv_rms * (scaled - x_send[i] * inner)).astype(jnp.bfloat16)


def write_out(dx_ref, dg_ref, dx_out, dg_out, sem):
    copies = [
        pltpu.make_async_copy(dg_ref, dg_out, sem.at[0]),
        pltpu.make_async_copy(dx_ref, dx_out, sem.at[1]),
    ]
    for copy in copies:
        copy.start()
    for copy in copies:
        copy.wait()


def fused(n_dp, n_tp, inputs, norm_gain, gate_grad, up_grad, gate_weight, up_weight):
    n = n_dp * n_tp
    seq, depth = gate_grad.shape[1:]
    width = gate_weight.shape[0]
    cut = width // n
    rows = n_dp * seq
    dma, vmem = pltpu.SemaphoreType.DMA, pltpu.VMEM
    input_grad, gain_grad = pl.pallas_call(
        functools.partial(kernel, n_dp, n_tp),
        out_shape=(vmem(inputs.shape, jnp.bfloat16), vmem((n, 1, cut), jnp.float32)),
        in_specs=[pl.BlockSpec(memory_space=pl.ANY)] * 6,
        out_specs=(pl.BlockSpec(memory_space=vmem),) * 2,
        scratch_shapes=[
            vmem((2 * n_tp * cut, depth), jnp.bfloat16),
            vmem((2, n_dp, seq, depth), jnp.bfloat16),
            vmem((2, rows, depth), jnp.bfloat16),
            vmem(inputs.shape, jnp.bfloat16),
            vmem((n, 1, cut), jnp.float32),
            vmem((n, 1, cut), jnp.float32),
            vmem((n, 1, cut), jnp.float32),
            vmem((n, cut), jnp.float32),
            vmem((n_tp // 2, cut, rows), jnp.float32),
            vmem((rows, cut), jnp.float32),
            vmem((n_tp, 1, cut), jnp.float32),
            vmem((n_tp, 1, cut), jnp.float32),
            vmem((n_tp, rows, cut), jnp.bfloat16),
            vmem((n_tp, rows, cut), jnp.bfloat16),
            vmem((n, 2, 1, cut), jnp.float32),
            vmem((n, 2, 1, cut), jnp.float32),
            dma((2,)), dma((4,)),
            pltpu.SemaphoreType.REGULAR((n_tp // 2 - 1,)),
            dma, dma((2,)),
            dma, dma,
            dma((2,)), dma((2, 3)),
            dma, dma,
        ],
        compiler_params=pltpu.CompilerParams(collective_id=0, has_side_effects=True),
    )(inputs, norm_gain.reshape(n, 1, cut), gate_grad, up_grad, gate_weight, up_weight)
    input_grad, gain_grad = pl.pallas_call(
        write_out,
        out_shape=(
            jax.ShapeDtypeStruct(inputs.shape, jnp.bfloat16),
            jax.ShapeDtypeStruct((n, 1, cut), jnp.float32),
        ),
        in_specs=[pl.BlockSpec(memory_space=vmem)] * 2,
        out_specs=(pl.BlockSpec(memory_space=pl.ANY),) * 2,
        scratch_shapes=[dma((2,))],
        compiler_params=pltpu.CompilerParams(vmem_limit_bytes=2**20),
    )(input_grad, gain_grad)
    return (input_grad, gain_grad.reshape(width))


def per_device(n_dp, n_tp, *args):
    inputs, gate_grad, gate_weight = args[0], args[2], args[4]
    n = n_dp * n_tp
    width, depth = gate_weight.shape
    fits = (
        inputs.shape[:2] == (1, 1)
        and gate_grad.shape[0] == 1
        and gate_grad.shape[1] == n_tp
        and n_tp % 8 == 0
        and n_tp & (n_tp - 1) == 0
        and width % (n * 128) == 0
        and depth % 256 == 0
        and width // n_dp * depth * 4 <= 40 * 2**20
    )
    return fused(n_dp, n_tp, *args) if fits else plain(*args)


def solution(mesh):
    return jax.shard_map(
        functools.partial(per_device, mesh.shape["dp"], mesh.shape["tp"]),
        mesh=mesh,
        in_specs=(
            P("dp", "tp", None),
            P(),
            P("dp", None, "tp"),
            P("dp", None, "tp"),
            P(None, "tp"),
            P(None, "tp"),
        ),
        out_specs=(P("dp", "tp", None), P()),
        check_vma=False,
    )
```

```python
import functools

import jax
import jax.numpy as jnp
from jax import lax
from jax.experimental import pallas as pl
from jax.experimental.pallas import tpu as pltpu
from jax.sharding import PartitionSpec as P

epsilon = 1e-05
MESH = pl.DeviceIdType.MESH
NT = (((1,), (1,)), ((), ()))


def normalize(values):
    inv_rms = lax.rsqrt(jnp.mean(values * values, axis=-1, keepdims=True) + epsilon)
    return (inv_rms, values * inv_rms)


def plain(inputs, norm_gain, gate_grad, up_grad, gate_weight, up_weight):
    seq = gate_grad.shape[1]
    width = gate_weight.shape[0]
    cot_gate = gate_grad.reshape(-1, gate_grad.shape[-1])
    cot_up = up_grad.reshape(-1, up_grad.shape[-1])
    inv_rms, normed = normalize(inputs.astype(jnp.float32))
    full_term = lax.dot_general(cot_gate, gate_weight, NT, preferred_element_type=jnp.float32)
    full_term = full_term + lax.dot_general(cot_up, up_weight, NT, preferred_element_type=jnp.float32)
    full_term = full_term.reshape(-1, seq, width)
    row_grad = lax.psum_scatter(full_term, "tp", scatter_dimension=1, tiled=True)
    gain_grad = lax.psum(jnp.sum(row_grad * normed, axis=(0, 1)), ("dp", "tp"))
    scaled = row_grad * norm_gain
    inner = jnp.mean(scaled * normed, axis=-1, keepdims=True)
    return ((inv_rms * (scaled - normed * inner)).astype(jnp.bfloat16), gain_grad)


def kernel(
    n_dp, n_tp, x_ref, gain_hbm, gg_ref, ug_ref, gw_ref, uw_ref, dx_ref, dg_ref,
    w_buf, cot, g_mat, x_row, gain_ref, x_send, x_recv, x_mat, acc, mine, scale_send, scale_recv, part_send, part_recv, last_send, last_recv,
    w_sem, own_sem, known, cot_ss, cot_rs, x_ss, x_rs, part_ss, part_rs, last_ss, last_rs,
):
    n = n_dp * n_tp
    bits = n_tp.bit_length() - 1
    d, t = lax.axis_index("dp"), lax.axis_index("tp")
    me = d * n_tp + t
    seq = gg_ref.shape[1]
    width = gw_ref.shape[0]
    cut = width // n
    base = d * (n_tp * cut)

    def flip(to, k):
        for bit in range(bits):
            if k >> bit & 1:
                to = to + 2**bit - 2 ** (bit + 1) * lax.rem(lax.div(to, 2**bit), 2)
        return to

    partners = [flip(t, k) for k in range(n_tp)]
    rows_of = [lax.rem(d + step, n_dp) for step in range(n_dp)]

    own = [
        pltpu.make_async_copy(gg_ref.at[0], cot.at[0, d], own_sem.at[0]),
        pltpu.make_async_copy(ug_ref.at[0], cot.at[1, d], own_sem.at[1]),
        pltpu.make_async_copy(x_ref, x_row, own_sem.at[2]),
        pltpu.make_async_copy(gain_hbm, gain_ref, own_sem.at[3]),
    ]
    with jax.named_scope("own_start"):
        for copy in own:
            copy.start(priority=1)

    spot, line = lax.div(t, 2), n_tp // 2
    beside = lax.min(spot, 1) + lax.min(line - 1 - spot, 1)

    def signal(sem, to_d, to_t):
        pl.semaphore_signal(sem, inc=1, device_id={"dp": to_d, "tp": to_t}, device_id_type=MESH)

    def signal_line(sem):
        @pl.when(spot > 0)
        def _():
            signal(sem, d, t - 2)

        @pl.when(spot < line - 1)
        def _():
            signal(sem, d, t + 2)

    with jax.named_scope("greet"):
        barrier = pltpu.get_barrier_semaphore()
        for step in range(1, n_dp):
            signal(barrier, rows_of[step], t)
        signal(barrier, d, partners[1])
        signal_line(barrier)

    order = sorted(range(n_tp), key=lambda k: -(k.bit_length()))
    half = n_tp // 2

    def first_far(i, which):
        return i < half and which == 0

    def weight_copy(i, which):
        rows = pl.ds(pl.multiple_of(base + partners[order[i]] * cut, cut), cut)
        source = (gw_ref, uw_ref)[which]
        slot = pl.ds((which * n_tp + i) * cut, cut)
        return pltpu.make_async_copy(source.at[rows, :], w_buf.at[slot, :], w_sem.at[0 if first_far(i, which) else 1])

    def weights_here(which):
        low, count = ((0, half), (half, 2 * n_tp - half))[which]
        return pltpu.make_async_copy(
            gw_ref.at[pl.ds(0, count * cut), :], w_buf.at[pl.ds(low * cut, count * cut), :], w_sem.at[which]
        )

    stream = [(i, 0) for i in range(half)] + [(i, 1) for i in range(half)]
    stream += [(i, which) for i in range(half, n_tp) for which in range(2)]
    with jax.named_scope("w_start"):
        for i, which in stream:
            weight_copy(i, which).start()

    def cot_copy(step, which):
        to = rows_of[step]
        return pltpu.make_async_remote_copy(
            src_ref=cot.at[which, d], dst_ref=cot.at[which, d], send_sem=cot_ss, recv_sem=cot_rs.at[which],
            device_id={"dp": to, "tp": t}, device_id_type=MESH,
        )

    def cots(which):
        return pltpu.make_async_remote_copy(
            src_ref=cot.at[which, pl.ds(0, n_dp - 1)], dst_ref=cot.at[which, pl.ds(0, n_dp - 1)], send_sem=cot_ss,
            recv_sem=cot_rs.at[which], device_id={"dp": rows_of[1], "tp": t}, device_id_type=MESH,
        )

    with jax.named_scope("own_wait"):
        own[0].wait()
        own[1].wait()
    with jax.named_scope("bar_wait"):
        pl.semaphore_wait(barrier, n_dp + beside)
    with jax.named_scope("cot_start"):
        for which in range(2):
            for step in range(1, n_dp):
                cot_copy(step, which).start()

    groups = [(0, half), (half, n_tp - 1)]

    def part_copies(i):
        group = [low <= i < high for low, high in groups].index(True)
        return [
            pltpu.make_async_remote_copy(
                src_ref=send.at[i], dst_ref=recv.at[i], send_sem=part_ss.at[which], recv_sem=part_rs.at[which, group],
                device_id={"dp": d, "tp": partners[order[i]]}, device_id_type=MESH,
            )
            for which, (send, recv) in enumerate(((scale_send, scale_recv), (part_send, part_recv)))
        ]

    def parts(low, high, group):
        return [
            pltpu.make_async_remote_copy(
                src_ref=send.at[pl.ds(low, high - low)], dst_ref=recv.at[pl.ds(low, high - low)],
                send_sem=part_ss.at[which], recv_sem=part_rs.at[which, group],
                device_id={"dp": d, "tp": partners[1]}, device_id_type=MESH,
            )
            for which, (send, recv) in enumerate(((scale_send, scale_recv), (part_send, part_recv)))
        ]

    place = t * n_dp + d

    def other(k):
        flat = k + lax.div(k + n - place, n)
        to_t = lax.div(flat, n_dp)
        return flat - to_t * n_dp, to_t

    def spread(send, recv, send_sem, recv_sem, to):
        to_d, to_t = to
        return pltpu.make_async_remote_copy(
            src_ref=send.at[to_d * n_tp + to_t], dst_ref=recv.at[me], send_sem=send_sem, recv_sem=recv_sem,
            device_id={"dp": to_d, "tp": to_t}, device_id_type=MESH,
        )

    def all_of(send, recv, send_sem, recv_sem):
        return pltpu.make_async_remote_copy(
            src_ref=send.at[pl.ds(0, n - 1)], dst_ref=recv.at[pl.ds(0, n - 1)], send_sem=send_sem,
            recv_sem=recv_sem, device_id={"dp": rows_of[1], "tp": t}, device_id_type=MESH,
        )

    def gather(which):
        cots(which).wait_recv()
        for row in range(n_dp):
            g_mat[which, row * seq:(row + 1) * seq, :] = cot[which, row]

    def encode(i, cols, part):
        most = jnp.maximum(jnp.max(jnp.abs(part), axis=0, keepdims=True), 1e-30)
        scale_send[i, :, cols] = most * 2.0**-15
        root = part * (2.0**15 / most)
        square = root * root
        fourth = square * square
        part_send[i, :, cols] = (fourth * square * root * jnp.abs(root)).astype(jnp.bfloat16)

    def decode(i):
        power = part_recv[i].astype(jnp.float32)
        back = lax.rsqrt(lax.rsqrt(lax.rsqrt(jnp.maximum(jnp.abs(power), 2.0**-126))))
        square = back * back
        return power * (square * square * square * back) * scale_recv[i]

    lanes = [slice(low, low + cut // 2) for low in range(0, cut, cut // 2)]

    def product(i, which, rows):
        low = (which * n_tp + i) * cut + rows.start
        return lax.dot_general(w_buf[low:low + cut // 2, :], g_mat[which], NT, preferred_element_type=jnp.float32)

    signal_line(known.at[1])
    signal(known.at[1], d, partners[1])
    with jax.named_scope("x_norm"):
        own[2].wait()
        squares = jnp.zeros((1, cut), jnp.float32)
        for i in range(n):
            piece = x_row[0, :, i * cut:(i + 1) * cut].astype(jnp.float32)
            x_send[i] = piece
            squares = squares + piece * piece
        inv_rms = lax.rsqrt(jnp.sum(squares, axis=1, keepdims=True) / width + epsilon)
        for i in range(n):
            x_send[i] = x_send[i] * inv_rms
        x_recv[me] = x_send[me]
    with jax.named_scope("rounds"):
        for step in range(1, line - 1):
            pl.semaphore_wait(known.at[step], beside + (1 if step == 1 else 0))
            if step + 1 < line - 1:
                signal_line(known.at[step + 1])
        for step in range(n_dp):
            for side in range(2):
                if step or side:
                    signal(known.at[0], rows_of[step], partners[side])
    with jax.named_scope("gather0"):
        gather(0)
        weights_here(0).wait()
    with jax.named_scope("gate_far"):
        for i in range(half):
            for rows in lanes:
                acc[i, rows, :] = product(i, 0, rows)
    with jax.named_scope("x_start"):
        pl.semaphore_wait(known.at[0], 2 * n_dp - 1)
        for side in range(n_tp):
            for step in range(n_dp):
                if side or step:
                    spread(x_send, x_recv, x_ss, x_rs, (rows_of[step], partners[n_tp - side if side else 0])).start()
    with jax.named_scope("gather1"):
        gather(1)
        weights_here(1).wait()
    with jax.named_scope("products"):
        for low, high in ((0, half // 2), (half // 2, half), (half, n_tp - 1), (n_tp - 1, n_tp)):
            for i in range(low, high):
                for rows in lanes:
                    if i < half:
                        part = (acc[i, rows, :] + product(i, 1, rows)).T
                    else:
                        part = (product(i, 0, rows) + product(i, 1, rows)).T
                    if i < n_tp - 1:
                        encode(i, rows, part)
                    else:
                        mine[:, rows] = part
            for i in range(low, min(high, n_tp - 1)):
                for copy in part_copies(i):
                    copy.start()
    total = mine[...]

    with jax.named_scope("x_wait"):
        all_of(x_send, x_recv, x_ss, x_rs).wait_recv()
    with jax.named_scope("x_mat"):
        for i in range(n):
            x_mat[i:i + 1, :] = x_recv[i]

    for group, (low, high) in enumerate(groups):
        with jax.named_scope(f"part{group}"):
            for copy in parts(low, high, group):
                copy.wait_recv()
            for i in range(low, high):
                total = total + decode(i)

    with jax.named_scope("gain_part"):
        gain_part = jnp.sum(total * x_mat[...], axis=0, keepdims=True)
        for i in range(n):
            last_send[i, 0] = total[i:i + 1, :]
            last_send[i, 1] = gain_part
    with jax.named_scope("last_start"):
        for k in range(n - 1):
            spread(last_send, last_recv, last_ss, last_rs, other(k)).start()

        last_recv[me] = last_send[me]

    with jax.named_scope("send_waits"):
        own[3].wait()
        for which in range(2):
            cots(which).wait_send()
        for copy in parts(0, n_tp - 1, 0):
            copy.wait_send()
        all_of(x_send, x_recv, x_ss, x_rs).wait_send()
        all_of(last_send, last_recv, last_ss, last_rs).wait_send()

    with jax.named_scope("last_wait"):
        all_of(last_send, last_recv, last_ss, last_rs).wait_recv()

    with jax.named_scope("finish"):
        dots = jnp.zeros((1, cut), jnp.float32)
        for i in range(n):
            dots = dots + last_recv[i, 0] * gain_ref[i] * x_send[i]
            dg_ref[i] = last_recv[i, 1]
        inner = jnp.sum(dots, axis=1, keepdims=True) / width
        for i in range(n):
            scaled = last_recv[i, 0] * gain_ref[i]
            dx_ref[0, :, i * cut:(i + 1) * cut] = (inv_rms * (scaled - x_send[i] * inner)).astype(jnp.bfloat16)


def write_out(dx_ref, dg_ref, dx_out, dg_out, sem):
    copies = [
        pltpu.make_async_copy(dg_ref, dg_out, sem.at[0]),
        pltpu.make_async_copy(dx_ref, dx_out, sem.at[1]),
    ]
    for copy in copies:
        copy.start()
    for copy in copies:
        copy.wait()


def fused(n_dp, n_tp, inputs, norm_gain, gate_grad, up_grad, gate_weight, up_weight):
    n = n_dp * n_tp
    seq, depth = gate_grad.shape[1:]
    width = gate_weight.shape[0]
    cut = width // n
    rows = n_dp * seq
    dma, vmem = pltpu.SemaphoreType.DMA, pltpu.VMEM
    input_grad, gain_grad = pl.pallas_call(
        functools.partial(kernel, n_dp, n_tp),
        out_shape=(vmem(inputs.shape, jnp.bfloat16), vmem((n, 1, cut), jnp.float32)),
        in_specs=[pl.BlockSpec(memory_space=pl.ANY)] * 6,
        out_specs=(pl.BlockSpec(memory_space=vmem),) * 2,
        scratch_shapes=[
            vmem((2 * n_tp * cut, depth), jnp.bfloat16),
            vmem((2, n_dp, seq, depth), jnp.bfloat16),
            vmem((2, rows, depth), jnp.bfloat16),
            vmem(inputs.shape, jnp.bfloat16),
            vmem((n, 1, cut), jnp.float32),
            vmem((n, 1, cut), jnp.float32),
            vmem((n, 1, cut), jnp.float32),
            vmem((n, cut), jnp.float32),
            vmem((n_tp // 2, cut, rows), jnp.float32),
            vmem((rows, cut), jnp.float32),
            vmem((n_tp, 1, cut), jnp.float32),
            vmem((n_tp, 1, cut), jnp.float32),
            vmem((n_tp, rows, cut), jnp.bfloat16),
            vmem((n_tp, rows, cut), jnp.bfloat16),
            vmem((n, 2, 1, cut), jnp.float32),
            vmem((n, 2, 1, cut), jnp.float32),
            dma((2,)), dma((4,)),
            pltpu.SemaphoreType.REGULAR((n_tp // 2 - 1,)),
            dma, dma((2,)),
            dma, dma,
            dma((2,)), dma((2, 2)),
            dma, dma,
        ],
        compiler_params=pltpu.CompilerParams(collective_id=0, has_side_effects=True),
    )(inputs, norm_gain.reshape(n, 1, cut), gate_grad, up_grad, gate_weight, up_weight)
    input_grad, gain_grad = pl.pallas_call(
        write_out,
        out_shape=(
            jax.ShapeDtypeStruct(inputs.shape, jnp.bfloat16),
            jax.ShapeDtypeStruct((n, 1, cut), jnp.float32),
        ),
        in_specs=[pl.BlockSpec(memory_space=vmem)] * 2,
        out_specs=(pl.BlockSpec(memory_space=pl.ANY),) * 2,
        scratch_shapes=[dma((2,))],
        compiler_params=pltpu.CompilerParams(vmem_limit_bytes=2**20),
    )(input_grad, gain_grad)
    return (input_grad, gain_grad.reshape(width))


def per_device(n_dp, n_tp, *args):
    inputs, gate_grad, gate_weight = args[0], args[2], args[4]
    n = n_dp * n_tp
    width, depth = gate_weight.shape
    fits = (
        inputs.shape[:2] == (1, 1)
        and gate_grad.shape[0] == 1
        and gate_grad.shape[1] == n_tp
        and n_tp % 8 == 0
        and n_tp & (n_tp - 1) == 0
        and width % (n * 128) == 0
        and depth % 256 == 0
        and width // n_dp * depth * 4 <= 40 * 2**20
    )
    return fused(n_dp, n_tp, *args) if fits else plain(*args)


def solution(mesh):
    return jax.shard_map(
        functools.partial(per_device, mesh.shape["dp"], mesh.shape["tp"]),
        mesh=mesh,
        in_specs=(
            P("dp", "tp", None),
            P(),
            P("dp", None, "tp"),
            P("dp", None, "tp"),
            P(None, "tp"),
            P(None, "tp"),
        ),
        out_specs=(P("dp", "tp", None), P()),
        check_vma=False,
    )
```
